32 devices in a mesh: ctx: 8 (over z, x), tp: 4 (over y, core).
Axes of the slice: x: 2, y: 2, z: 4, core: 2. Of those that a mesh axis runs over, the one named last changes fastest.
Arguments:
- queries: bfloat16 [1024, 8192], P(('ctx', 'tp')), may hold values from -6 to 6
- keys: bfloat16 [1024, 1024], P(('ctx', 'tp')), may hold values from -6 to 6
- values: bfloat16 [1024, 1024], P(('ctx', 'tp')), may hold values from -6 to 6
- doc_starts: int32 [14], replicated, may hold values from 0 to 1024, as said below
Outputs:
- attended: bfloat16 [1024, 8192], P(('ctx', 'tp'))
The draws below stay inside these ranges and needn't reach their ends.
Inputs may be any that keep to these rules, and one draw needn't show every extreme that they name: `doc_starts`: nondecreasing and starting with 0; consecutive entries differ by at most 384, and some pair of consecutive entries below 1024 differs by exactly 384; the last document ends at 1024, and entries equal to 1024 stand for empty documents.
All inputs are finite; a program needn't handle non-finite values.
Results may differ from the reference program's by a relative error of at most 0.004.
Values may be sent and summed in bfloat16 or wider, within the bound.
A program may use at most 64 MiB of HBM per device.

```python
import jax
import jax.numpy as jnp
from jax import lax

QUERY_HEAD_COUNT = 64
KEY_VALUE_HEADS = 8
HEAD_WIDTH = 128
TOK_DEV = 32
PACKED_TOKENS = 1024
MOST = 384
NDOCS = 14
N_CTX = 8
N_TP = 4


def draw_queries(key, part):
    start_offset = jnp.clip(jax.random.normal(jax.random.fold_in(key, 1), (PACKED_TOKENS, QUERY_HEAD_COUNT * HEAD_WIDTH), jnp.float32), -5.0, 5.0)
    return start_offset.astype(jnp.bfloat16)


def draw_keys(key, part):
    start_offset = jnp.clip(jax.random.normal(jax.random.fold_in(key, 2), (PACKED_TOKENS, KEY_VALUE_HEADS * HEAD_WIDTH), jnp.float32), -5.0, 5.0)
    return start_offset.astype(jnp.bfloat16)


def draw_doc_starts(key, part):
    lowest = MOST // 4
    spread = MOST - lowest
    first_draw = jax.random.randint(jax.random.fold_in(key, 21), (NDOCS,), 0, spread + 1, dtype=jnp.int32)
    second_draw = jax.random.randint(jax.random.fold_in(key, 22), (NDOCS,), 0, spread + 1, dtype=jnp.int32)
    lengths = lowest + first_draw * second_draw // spread
    chosen = jax.random.randint(jax.random.fold_in(key, 23), (), 0, PACKED_TOKENS // MOST - 1, dtype=jnp.int32)
    lengths = jnp.where(jnp.arange(NDOCS, dtype=jnp.int32) == chosen, MOST, lengths).astype(jnp.int32)
    ends = jnp.cumsum(lengths).astype(jnp.int32)
    starts = jnp.concatenate([jnp.zeros((1,), jnp.int32), ends[:-1]])
    return jnp.minimum(starts, PACKED_TOKENS).astype(jnp.int32)


def levels(key, extent, pieces, smallest, high):
    loudness = 1.0
    for axis_at, parts in pieces:
        heights = jax.random.uniform(jax.random.fold_in(jax.random.fold_in(key, 6), axis_at), (parts,), jnp.float32, smallest / len(pieces), high / len(pieces))
        loudness = loudness * jnp.repeat(jnp.exp(heights), extent[axis_at] // parts).reshape((-1,) + (1,) * (len(extent) - 1 - axis_at))
    return loudness


def normal_values(stream_key, extent, scale, reach, cuts=(), held_as=jnp.bfloat16):
    entries = jax.random.normal(stream_key, extent, jnp.float32) * scale
    if len(cuts) > 0:
        entries = levels(stream_key, extent, cuts, -0.22, 0.18) * entries
    return jnp.clip(entries, min=-reach, max=reach).astype(held_as)


def setup_inputs(seed: int = 0) -> dict:
    arg_keys = jax.random.split(jax.random.key(seed), 5)
    queries = draw_queries(jax.random.fold_in(arg_keys[4], 71), 0)
    keys = draw_keys(jax.random.fold_in(arg_keys[4], 71), 0)
    values = normal_values(arg_keys[2], (PACKED_TOKENS, KEY_VALUE_HEADS * HEAD_WIDTH), 1.0, 6.0, ((0, 32),))
    doc_starts = draw_doc_starts(jax.random.fold_in(arg_keys[4], 71), 0)
    return dict(queries=queries, keys=keys, values=values, doc_starts=doc_starts)


def doc_begin(positions, doc_starts):
    found = jnp.where(doc_starts[None, :] <= positions[:, None], doc_starts[None, :], 0)
    return jnp.max(found, axis=1)


def reference(queries, keys, values, doc_starts):
    rows_per_block = TOK_DEV * N_TP
    reach_blocks = min(8, N_CTX // 2)
    visible_span = reach_blocks * rows_per_block
    query_groups = QUERY_HEAD_COUNT // KEY_VALUE_HEADS
    scale = HEAD_WIDTH ** -0.5
    leading_count = (reach_blocks - 1) * rows_per_block
    padded_key_rows = jnp.concatenate([jnp.zeros((leading_count, KEY_VALUE_HEADS * HEAD_WIDTH), jnp.bfloat16), keys], axis=0)
    padded_value_rows = jnp.concatenate([jnp.zeros((leading_count, KEY_VALUE_HEADS * HEAD_WIDTH), jnp.bfloat16), values], axis=0)

    def one_block(index):
        leading_entry = (index * rows_per_block).astype(jnp.int32)
        query_matrix = lax.dynamic_slice_in_dim(queries, leading_entry, rows_per_block, 0)
        query_matrix = query_matrix.reshape(rows_per_block, KEY_VALUE_HEADS, query_groups, HEAD_WIDTH).astype(jnp.float32)
        key_matrix = lax.dynamic_slice_in_dim(padded_key_rows, leading_entry, visible_span, 0).reshape(visible_span, KEY_VALUE_HEADS, HEAD_WIDTH).astype(jnp.float32)
        value_matrix = lax.dynamic_slice_in_dim(padded_value_rows, leading_entry, visible_span, 0).reshape(visible_span, KEY_VALUE_HEADS, HEAD_WIDTH).astype(jnp.float32)
        scores = jnp.einsum("qkgd,pkd->kgqp", query_matrix, key_matrix) * scale
        query_pos = leading_entry + jnp.arange(rows_per_block, dtype=jnp.int32)
        key_pos = leading_entry - leading_count + jnp.arange(visible_span, dtype=jnp.int32)
        begins = doc_begin(query_pos, doc_starts)
        visible = (key_pos[None, :] <= query_pos[:, None]) & (key_pos[None, :] >= begins[:, None])
        scores = jnp.where(visible, scores, -1e30)
        top = jnp.max(scores, axis=-1, keepdims=True)
        probs = jnp.where(visible, jnp.exp(scores - top), 0.0)
        denom = jnp.sum(probs, axis=-1)
        rounded = lax.optimization_barrier(probs.astype(jnp.bfloat16)).astype(jnp.float32)
        numer = jnp.einsum("kgqp,pkd->kgqd", rounded, value_matrix)
        result = numer / denom[..., None]
        result = jnp.transpose(result, (2, 0, 1, 3)).reshape(rows_per_block, QUERY_HEAD_COUNT * HEAD_WIDTH)
        return result.astype(jnp.bfloat16)

    blocks = lax.map(one_block, jnp.arange(N_CTX, dtype=jnp.int32))
    return blocks.reshape(PACKED_TOKENS, QUERY_HEAD_COUNT * HEAD_WIDTH)
```

```python
import functools
import math

import jax
import jax.numpy as jnp
from jax import lax
from jax.experimental import pallas as pl
from jax.experimental.pallas import tpu as pltpu
from jax.sharding import PartitionSpec as P

QUERY_HEAD_COUNT = 64
KEY_VALUE_HEADS = 8
HEAD_WIDTH = 128
CORES = 2
MESH = pl.DeviceIdType.MESH


def plan(n_ctx, n_tp):
    span = n_tp // CORES
    across = span if n_ctx % span == 0 else 1
    in_plane = span * across
    planes = n_ctx * n_tp // CORES // in_plane
    reach_blocks = min(8, n_ctx // 2)
    reach = (reach_blocks - 1) * n_tp // CORES
    return in_plane, planes, reach


def kernel(n_ctx, n_tp, n_docs, docs, q_hbm, k_hbm, v_hbm, o_ref, q_buf, kv, bias, local_sem, send_sem, recv_sem):
    in_plane, planes, reach = plan(n_ctx, n_tp)
    levels = (reach + in_plane - 1) // in_plane
    rows = k_hbm.shape[0]
    width = k_hbm.shape[1]
    me = lax.axis_index("ctx") * n_tp + lax.axis_index("tp")
    core, chip = lax.rem(me, CORES), lax.div(me, CORES)
    plane, spot = lax.div(chip, in_plane), lax.rem(chip, in_plane)

    def device(other_chip, other_core):
        index = other_chip * CORES + other_core
        return (lax.div(index, n_tp), lax.rem(index, n_tp))

    def piece(distance, from_core):
        return CORES * (reach - distance) + from_core

    transit = CORES * (reach + 1)

    def part(index):
        return kv.at[pl.ds(pl.multiple_of(index * rows, rows), rows), :]

    own = piece(0, core)
    own_rows = pl.ds(pl.multiple_of(own * rows, rows), rows)
    load_k = pltpu.make_async_copy(k_hbm, kv.at[own_rows, pl.ds(0, width)], local_sem.at[0])
    load_v = pltpu.make_async_copy(v_hbm, kv.at[own_rows, pl.ds(width, width)], local_sem.at[1])
    load_q = pltpu.make_async_copy(q_hbm, q_buf, local_sem.at[2])
    load_k.start()
    load_v.start()
    load_q.start()

    partner = device(chip, 1 - core)
    around = [lax.rem(spot + o, in_plane) for o in range(1, in_plane)]
    barrier = pltpu.get_barrier_semaphore()
    pl.semaphore_signal(barrier, inc=1, device_id=partner, device_id_type=MESH)
    for other in around:
        pl.semaphore_signal(
            barrier, inc=1, device_id=device(plane * in_plane + other, core), device_id_type=MESH
        )
    below, above = plane > 0, plane < planes - 1

    @pl.when(below)
    def _():
        pl.semaphore_signal(
            barrier, inc=1, device_id=device(chip - in_plane, core), device_id_type=MESH
        )

    @pl.when(above)
    def _():
        pl.semaphore_signal(
            barrier, inc=1, device_id=device(chip + in_plane, core), device_id_type=MESH
        )

    sent = []

    def send(when, source, target, target_index):
        copy = pltpu.make_async_remote_copy(
            src_ref=part(source),
            dst_ref=part(target_index),
            send_sem=send_sem.at[len(sent)],
            recv_sem=recv_sem.at[target_index],
            device_id=target,
            device_id_type=MESH,
        )
        sent.append((when, copy))
        pl.when(when)(copy.start)

    def arrived(when, index):
        copy = pltpu.make_async_copy(part(index), part(index), recv_sem.at[index])
        pl.when(when)(copy.wait)

    for distance in range(1, reach + 1):
        @pl.when(chip < distance)
        def _():
            first = piece(distance, 0) * rows
            kv[pl.ds(first, CORES * rows), :] = jnp.zeros((CORES * rows, 2 * width), kv.dtype)

    pl.semaphore_wait(
        barrier, in_plane + below.astype(jnp.int32) + above.astype(jnp.int32)
    )
    load_k.wait()
    load_v.wait()

    def forwards(level, source, held):
        distance = level * in_plane
        if level < levels:
            following = distance + in_plane
            index = piece(following, core) if following <= reach else transit + core
            needed = following - spot <= reach
            send(held & above & needed, source, device(chip + in_plane, core), index)
        for other in around:
            away = distance + other - spot
            send(
                held & (away >= 1) & (away <= reach),
                source,
                device(plane * in_plane + other, core),
                piece(jnp.clip(away, 1, reach), core),
            )
        if distance <= reach:
            send(held, source, partner, piece(distance, core))

    def pass_to_partner(when, distance):
        index = piece(distance, core)
        arrived(when, index)
        send(when, index, partner, index)

    forwards(0, own, chip >= 0)

    keys = CORES * rows * (reach + 1)
    query_pos = me * rows + lax.broadcasted_iota(jnp.int32, (rows, keys), 0)
    key_pos = (chip - reach) * (CORES * rows) + lax.broadcasted_iota(jnp.int32, (rows, keys), 1)
    token = me * rows + lax.broadcasted_iota(jnp.int32, (rows, 1), 0)
    begin = jnp.zeros((rows, 1), jnp.int32)
    for doc in range(n_docs):
        start = docs[doc]
        begin = jnp.maximum(begin, jnp.where(start <= token, start, 0))
    visible = (key_pos <= query_pos) & (key_pos >= begin)
    bias[...] = jnp.where(visible, 0.0, -1e30)
    load_q.wait()

    for level in range(1, levels + 1):
        distance = level * in_plane
        index = piece(distance, core) if distance <= reach else transit + core
        held = (plane >= level) & (distance - spot <= reach)
        if level > 1:
            for back in range(1, min(reach, (level - 1) * in_plane - 1) + 1):
                if back % in_plane:
                    origin = lax.div(spot - back + 4 * in_plane, in_plane) - 4
                    pass_to_partner((chip >= back) & (origin == 2 - level), back)
        arrived(held, index)
        forwards(level, index, held)
    for back in range(1, reach + 1):
        if back % in_plane:
            origin = lax.div(spot - back + 4 * in_plane, in_plane) - 4
            pass_to_partner((chip >= back) & (origin <= 1 - levels), back)
    for distance in range(reach + 1):
        arrived(chip >= distance, piece(distance, 1 - core))

    group = QUERY_HEAD_COUNT // KEY_VALUE_HEADS
    factor = HEAD_WIDTH ** (-0.5) * math.log2(math.e)

    def head(g, carry):
        first = pl.multiple_of(g * (group * HEAD_WIDTH), group * HEAD_WIDTH)
        queries = jnp.concatenate(
            [q_buf[:, pl.ds(first + h * HEAD_WIDTH, HEAD_WIDTH)] for h in range(group)], axis=0
        )
        at = pl.multiple_of(g * HEAD_WIDTH, HEAD_WIDTH)
        key = kv[pl.ds(0, keys), pl.ds(at, HEAD_WIDTH)]
        value = kv[pl.ds(0, keys), pl.ds(width + at, HEAD_WIDTH)]
        scores = lax.dot_general(
            queries, key, (((1,), (1,)), ((), ())), preferred_element_type=jnp.float32
        )
        scores = (scores.reshape(group, rows, keys) + bias[...][None]).reshape(group * rows, keys)
        top = jnp.max(scores, axis=1, keepdims=True)
        probs = jnp.exp2((scores - top) * factor)
        total = jnp.sum(probs, axis=1, keepdims=True)
        out = jnp.dot(probs.astype(jnp.bfloat16), value, preferred_element_type=jnp.float32)
        out = (out / total).astype(jnp.bfloat16)
        for h in range(group):
            o_ref[:, pl.ds(first + h * HEAD_WIDTH, HEAD_WIDTH)] = out[h * rows : (h + 1) * rows]
        return carry

    lax.fori_loop(0, KEY_VALUE_HEADS, head, 0)
    for when, copy in sent:
        pl.when(when)(copy.wait_send)


def body(n_ctx, n_tp, queries, keys, values, doc_starts):
    in_plane, planes, reach = plan(n_ctx, n_tp)
    levels = (reach + in_plane - 1) // in_plane
    rows, width = keys.shape
    pieces = CORES * (reach + 2)
    copies = (levels + 1) * (in_plane + 1) + levels * (reach + 1)
    return pl.pallas_call(
        functools.partial(kernel, n_ctx, n_tp, doc_starts.shape[0]),
        out_shape=jax.ShapeDtypeStruct(queries.shape, queries.dtype),
        in_specs=[pl.BlockSpec(memory_space=pltpu.SMEM)]
        + [pl.BlockSpec(memory_space=pl.ANY)] * 3,
        out_specs=pl.BlockSpec(memory_space=pltpu.VMEM),
        scratch_shapes=[
            pltpu.VMEM(queries.shape, queries.dtype),
            pltpu.VMEM((pieces * rows, 2 * width), keys.dtype),
            pltpu.VMEM((rows, CORES * rows * (reach + 1)), jnp.float32),
            pltpu.SemaphoreType.DMA((3,)),
            pltpu.SemaphoreType.DMA((copies,)),
            pltpu.SemaphoreType.DMA((pieces,)),
        ],
        compiler_params=pltpu.CompilerParams(collective_id=0, has_side_effects=True),
    )(doc_starts, queries, keys, values)


def solution(mesh):
    n_ctx, n_tp = mesh.shape["ctx"], mesh.shape["tp"]
    in_specs = (P(("ctx", "tp"), None), P(("ctx", "tp"), None), P(("ctx", "tp"), None), P())
    return jax.shard_map(
        functools.partial(body, n_ctx, n_tp),
        mesh=mesh,
        in_specs=in_specs,
        out_specs=P(("ctx", "tp"), None),
        check_vma=False,
    )
```

```python
import functools
import math

import jax
import jax.numpy as jnp
from jax import lax
from jax.experimental import pallas as pl
from jax.experimental.pallas import tpu as pltpu
from jax.sharding import PartitionSpec as P

QUERY_HEAD_COUNT = 64
KEY_VALUE_HEADS = 8
HEAD_WIDTH = 128
CORES = 2
ROW_CUTS = 2
CHUNKS = 2 * ROW_CUTS
MESH = pl.DeviceIdType.MESH


def plan(n_ctx, n_tp):
    span = n_tp // CORES
    across = span if n_ctx % span == 0 else 1
    in_plane = span * across
    planes = n_ctx * n_tp // CORES // in_plane
    reach_blocks = min(8, n_ctx // 2)
    reach = (reach_blocks - 1) * n_tp // CORES
    return in_plane, planes, reach


def kernel(n_ctx, n_tp, n_docs, docs, q_hbm, k_hbm, v_hbm, o_ref, q_buf, kv, bias, local_sem, send_sem, recv_sem):
    in_plane, planes, reach = plan(n_ctx, n_tp)
    levels = (reach + in_plane - 1) // in_plane
    rows = k_hbm.shape[0]
    width = k_hbm.shape[1]
    me = lax.axis_index("ctx") * n_tp + lax.axis_index("tp")
    core, chip = lax.rem(me, CORES), lax.div(me, CORES)
    plane, spot = lax.div(chip, in_plane), lax.rem(chip, in_plane)

    def device(other_chip, other_core):
        index = other_chip * CORES + other_core
        return (lax.div(index, n_tp), lax.rem(index, n_tp))

    def piece(distance, from_core):
        return CORES * (reach - distance) + from_core

    transit = CORES * (reach + 1)

    tall = rows // ROW_CUTS

    def part(index, chunk):
        cut, side = chunk % ROW_CUTS, chunk // ROW_CUTS
        return kv.at[
            pl.ds(pl.multiple_of(index * rows + cut * tall, tall), tall),
            pl.ds(side * width, width),
        ]

    own = piece(0, core)
    own_rows = pl.ds(pl.multiple_of(own * rows, rows), rows)
    load_k = pltpu.make_async_copy(k_hbm, kv.at[own_rows, pl.ds(0, width)], local_sem.at[0])
    load_v = pltpu.make_async_copy(v_hbm, kv.at[own_rows, pl.ds(width, width)], local_sem.at[1])
    load_q = pltpu.make_async_copy(q_hbm, q_buf, local_sem.at[2])
    load_k.start()
    load_v.start()
    load_q.start()

    partner = device(chip, 1 - core)
    around = [lax.rem(spot + o, in_plane) for o in range(1, in_plane)]
    barrier = pltpu.get_barrier_semaphore()
    pl.semaphore_signal(barrier, inc=1, device_id=partner, device_id_type=MESH)
    for other in around:
        pl.semaphore_signal(
            barrier, inc=1, device_id=device(plane * in_plane + other, core), device_id_type=MESH
        )
    below, above = plane > 0, plane < planes - 1

    @pl.when(below)
    def _():
        pl.semaphore_signal(
            barrier, inc=1, device_id=device(chip - in_plane, core), device_id_type=MESH
        )

    @pl.when(above)
    def _():
        pl.semaphore_signal(
            barrier, inc=1, device_id=device(chip + in_plane, core), device_id_type=MESH
        )

    sent = []

    def send(when, chunk, source, target, target_index):
        copy = pltpu.make_async_remote_copy(
            src_ref=part(source, chunk),
            dst_ref=part(target_index, chunk),
            send_sem=send_sem.at[len(sent)],
            recv_sem=recv_sem.at[target_index, chunk],
            device_id=target,
            device_id_type=MESH,
        )
        sent.append((when, copy))
        pl.when(when)(copy.start)

    def arrived(when, index, chunk):
        place = part(index, chunk)
        copy = pltpu.make_async_copy(place, place, recv_sem.at[index, chunk])
        pl.when(when)(copy.wait)

    for distance in range(1, reach + 1):
        @pl.when(chip < distance)
        def _():
            first = piece(distance, 0) * rows
            kv[pl.ds(first, CORES * rows), :] = jnp.zeros((CORES * rows, 2 * width), kv.dtype)

    pl.semaphore_wait(
        barrier, in_plane + below.astype(jnp.int32) + above.astype(jnp.int32)
    )

    def forwards(level, source, held, chunk):
        distance = level * in_plane
        if level < levels:
            following = distance + in_plane
            index = piece(following, core) if following <= reach else transit + core
            needed = following - spot <= reach
            send(held & above & needed, chunk, source, device(chip + in_plane, core), index)
        for other in around:
            away = distance + other - spot
            send(
                held & (away >= 1) & (away <= reach),
                chunk,
                source,
                device(plane * in_plane + other, core),
                piece(jnp.clip(away, 1, reach), core),
            )
        if distance <= reach:
            send(held, chunk, source, partner, piece(distance, core))

    def pass_to_partner(when, distance):
        index = piece(distance, core)
        for chunk in range(CHUNKS):
            arrived(when, index, chunk)
            send(when, chunk, index, partner, index)

    load_k.wait()
    for chunk in range(CHUNKS):
        if chunk == ROW_CUTS:
            load_v.wait()
        forwards(0, own, chip >= 0, chunk)

    keys = CORES * rows * (reach + 1)
    query_pos = me * rows + lax.broadcasted_iota(jnp.int32, (rows, keys), 0)
    key_pos = (chip - reach) * (CORES * rows) + lax.broadcasted_iota(jnp.int32, (rows, keys), 1)
    token = me * rows + lax.broadcasted_iota(jnp.int32, (rows, 1), 0)
    begin = jnp.zeros((rows, 1), jnp.int32)
    for doc in range(n_docs):
        start = docs[doc]
        begin = jnp.maximum(begin, jnp.where(start <= token, start, 0))
    visible = (key_pos <= query_pos) & (key_pos >= begin)
    bias[...] = jnp.where(visible, 0.0, -1e30)
    load_q.wait()

    for level in range(1, levels + 1):
        distance = level * in_plane
        index = piece(distance, core) if distance <= reach else transit + core
        held = (plane >= level) & (distance - spot <= reach)
        if level > 1:
            for back in range(1, min(reach, (level - 1) * in_plane - 1) + 1):
                if back % in_plane:
                    origin = lax.div(spot - back + 4 * in_plane, in_plane) - 4
                    pass_to_partner((chip >= back) & (origin == 2 - level), back)
        for chunk in range(CHUNKS):
            arrived(held, index, chunk)
            forwards(level, index, held, chunk)
    for back in range(1, reach + 1):
        if back % in_plane:
            origin = lax.div(spot - back + 4 * in_plane, in_plane) - 4
            pass_to_partner((chip >= back) & (origin <= 1 - levels), back)
    for distance in range(reach + 1):
        for chunk in range(CHUNKS):
            arrived(chip >= distance, piece(distance, 1 - core), chunk)

    group = QUERY_HEAD_COUNT // KEY_VALUE_HEADS
    factor = HEAD_WIDTH ** (-0.5) * math.log2(math.e)

    ones = jnp.ones((keys, HEAD_WIDTH), jnp.bfloat16)
    hidden = bias[...][None]
    for g in range(KEY_VALUE_HEADS):
        first = g * group * HEAD_WIDTH
        queries = jnp.concatenate(
            [q_buf[:, pl.ds(first + h * HEAD_WIDTH, HEAD_WIDTH)] for h in range(group)], axis=0
        )
        key = kv[pl.ds(0, keys), pl.ds(g * HEAD_WIDTH, HEAD_WIDTH)]
        value = kv[pl.ds(0, keys), pl.ds(width + g * HEAD_WIDTH, HEAD_WIDTH)]
        scores = lax.dot_general(
            queries, key, (((1,), (1,)), ((), ())), preferred_element_type=jnp.float32
        )
        scores = (scores.reshape(group, rows, keys) + hidden).reshape(group * rows, keys)
        top = jnp.max(scores, axis=1, keepdims=True)
        probs = jnp.exp2((scores - top) * factor).astype(jnp.bfloat16)
        both = jnp.dot(
            probs, jnp.concatenate([value, ones], axis=1), preferred_element_type=jnp.float32
        )
        out = (both[:, :HEAD_WIDTH] / both[:, HEAD_WIDTH:]).astype(jnp.bfloat16)
        for h in range(group):
            o_ref[:, pl.ds(first + h * HEAD_WIDTH, HEAD_WIDTH)] = out[h * rows : (h + 1) * rows]
    for when, copy in sent:
        pl.when(when)(copy.wait_send)


def body(n_ctx, n_tp, queries, keys, values, doc_starts):
    in_plane, planes, reach = plan(n_ctx, n_tp)
    levels = (reach + in_plane - 1) // in_plane
    rows, width = keys.shape
    pieces = CORES * (reach + 2)
    copies = (levels + 1) * (in_plane + 1) + levels * (reach + 1)
    return pl.pallas_call(
        functools.partial(kernel, n_ctx, n_tp, doc_starts.shape[0]),
        out_shape=jax.ShapeDtypeStruct(queries.shape, queries.dtype),
        in_specs=[pl.BlockSpec(memory_space=pltpu.SMEM)]
        + [pl.BlockSpec(memory_space=pltpu.HBM)] * 3,
        out_specs=pl.BlockSpec(memory_space=pltpu.VMEM),
        scratch_shapes=[
            pltpu.VMEM(queries.shape, queries.dtype),
            pltpu.VMEM((pieces * rows, 2 * width), keys.dtype),
            pltpu.VMEM((rows, CORES * rows * (reach + 1)), jnp.float32),
            pltpu.SemaphoreType.DMA((3,)),
            pltpu.SemaphoreType.DMA((copies * CHUNKS,)),
            pltpu.SemaphoreType.DMA((pieces, CHUNKS)),
        ],
        compiler_params=pltpu.CompilerParams(collective_id=0, has_side_effects=True, vmem_limit_bytes=16 << 20),
    )(doc_starts, queries, keys, values)


def solution(mesh):
    n_ctx, n_tp = mesh.shape["ctx"], mesh.shape["tp"]
    in_specs = (P(("ctx", "tp"), None), P(("ctx", "tp"), None), P(("ctx", "tp"), None), P())
    return jax.shard_map(
        functools.partial(body, n_ctx, n_tp),
        mesh=mesh,
        in_specs=in_specs,
        out_specs=P(("ctx", "tp"), None),
        check_vma=False,
    )
```

```python
import functools
import math

import jax
import jax.numpy as jnp
from jax import lax
from jax.experimental import pallas as pl
from jax.experimental.pallas import tpu as pltpu
from jax.sharding import PartitionSpec as P

QUERY_HEAD_COUNT = 64
KEY_VALUE_HEADS = 8
HEAD_WIDTH = 128
CORES = 2
ROW_CUTS = 2
CHUNKS = 2 * ROW_CUTS
VMEM_BYTES = 67043328 - 540 * 1024
MESH = pl.DeviceIdType.MESH


def plan(n_ctx, n_tp):
    deep = n_tp // CORES
    across = deep if n_ctx % deep == 0 else 1
    return deep, across, n_ctx // across, min(8, n_ctx // 2) - 1


def kernel(n_ctx, n_tp, n_docs, docs, q_hbm, k_hbm, v_hbm, o_ref, q_buf, kv, bias, local_sem, send_sem, recv_sem):
    deep, across, planes, lines = plan(n_ctx, n_tp)
    in_plane, reach = deep * across, lines * deep
    rows = k_hbm.shape[0]
    width = k_hbm.shape[1]
    me = lax.axis_index("ctx") * n_tp + lax.axis_index("tp")
    core, chip = lax.rem(me, CORES), lax.div(me, CORES)
    plane, x = lax.div(chip, in_plane), lax.rem(lax.div(chip, deep), across)
    y = lax.rem(chip, deep)

    def device(other_chip, other_core):
        index = other_chip * CORES + other_core
        return (lax.div(index, n_tp), lax.rem(index, n_tp))

    def piece(distance, from_core):
        return CORES * (reach - distance) + from_core

    tall = rows // ROW_CUTS

    def part(index, chunk):
        cut, side = chunk % ROW_CUTS, chunk // ROW_CUTS
        return kv.at[
            pl.ds(pl.multiple_of(index * rows + cut * tall, tall), tall),
            pl.ds(side * width, width),
        ]

    own = piece(0, core)
    own_rows = pl.ds(pl.multiple_of(own * rows, rows), rows)
    load_k = pltpu.make_async_copy(k_hbm, kv.at[own_rows, pl.ds(0, width)], local_sem.at[0])
    load_v = pltpu.make_async_copy(v_hbm, kv.at[own_rows, pl.ds(width, width)], local_sem.at[1])
    load_q = pltpu.make_async_copy(q_hbm, q_buf, local_sem.at[2])
    load_k.start()
    load_v.start()
    load_q.start()

    partner = device(chip, 1 - core)
    other_x = [lax.rem(x + o, across) for o in range(1, across)]
    other_y = [lax.rem(y + o, deep) for o in range(1, deep)]
    peers = [partner]
    peers += [device(chip + (other - x) * deep, core) for other in other_x]
    peers += [device(chip + other - y, core) for other in other_y]
    barrier = pltpu.get_barrier_semaphore()
    for peer in peers:
        pl.semaphore_signal(barrier, inc=1, device_id=peer, device_id_type=MESH)
    below, above = plane > 0, plane < planes - 1

    @pl.when(below)
    def _():
        pl.semaphore_signal(
            barrier, inc=1, device_id=device(chip - in_plane, core), device_id_type=MESH
        )

    @pl.when(above)
    def _():
        pl.semaphore_signal(
            barrier, inc=1, device_id=device(chip + in_plane, core), device_id_type=MESH
        )

    sent = []

    def send(when, chunk, source, target, target_index):
        copy = pltpu.make_async_remote_copy(
            src_ref=part(source, chunk),
            dst_ref=part(target_index, chunk),
            send_sem=send_sem.at[len(sent)],
            recv_sem=recv_sem.at[target_index, chunk],
            device_id=target,
            device_id_type=MESH,
        )
        sent.append((when, copy))
        pl.when(when)(copy.start)

    def arrived(when, index, chunk):
        place = part(index, chunk)
        copy = pltpu.make_async_copy(place, place, recv_sem.at[index, chunk])
        pl.when(when)(copy.wait)

    for distance in range(1, reach + 1):
        @pl.when(chip < distance)
        def _():
            first = piece(distance, 0) * rows
            kv[pl.ds(first, CORES * rows), :] = jnp.zeros((CORES * rows, 2 * width), kv.dtype)

    pl.semaphore_wait(
        barrier, len(peers) + below.astype(jnp.int32) + above.astype(jnp.int32)
    )

    def hand_on(line, chunk):
        index = piece(line * deep, core)
        held = chip >= line * deep
        if line + across <= lines:
            straight = held if line == 0 else held & (line > x)
            send(straight & above, chunk, index, device(chip + in_plane, core),
                 piece((line + across) * deep, core))
        if line in (0, across):
            for other in other_x:
                away = line + other - x
                send(held & (away >= 1) & (away <= lines), chunk, index,
                     device(chip + (other - x) * deep, core),
                     piece(jnp.clip(away, 1, lines) * deep, core))
        for other in other_y:
            away = line * deep + other - y
            send(held & (away >= 1) & (away <= reach), chunk, index,
                 device(chip + other - y, core), piece(jnp.clip(away, 1, reach), core))
        send(held, chunk, index, partner, index)

    def line_in(line):
        for chunk in range(CHUNKS):
            arrived(chip >= line * deep, piece(line * deep, core), chunk)
            hand_on(line, chunk)

    def beside(line):
        for off in range(1 - deep, deep):
            back = line * deep + off
            if off and 1 <= back <= reach:
                when = (chip >= back) & (y - off >= 0) & (y - off < deep)
                index = piece(back, core)
                for chunk in range(CHUNKS):
                    arrived(when, index, chunk)
                    send(when, chunk, index, partner, index)

    load_k.wait()
    for chunk in range(CHUNKS):
        if chunk == ROW_CUTS:
            load_v.wait()
        hand_on(0, chunk)

    keys = CORES * rows * (reach + 1)
    query_pos = me * rows + lax.broadcasted_iota(jnp.int32, (rows, keys), 0)
    key_pos = (chip - reach) * (CORES * rows) + lax.broadcasted_iota(jnp.int32, (rows, keys), 1)
    token = me * rows + lax.broadcasted_iota(jnp.int32, (rows, 1), 0)
    begin = jnp.zeros((rows, 1), jnp.int32)
    for doc in range(n_docs):
        start = docs[doc]
        begin = jnp.maximum(begin, jnp.where(start <= token, start, 0))
    visible = (key_pos <= query_pos) & (key_pos >= begin)
    bias[...] = jnp.where(visible, 0.0, -1e30)
    load_q.wait()

    line_in(across)
    beside(0)
    for line in range(1, across):
        line_in(line)
    beside(across)
    for line in range(across + 1, lines + 1):
        line_in(line)
    for line in range(1, lines + 1):
        if line != across:
            beside(line)
    for distance in range(reach + 1):
        for chunk in range(CHUNKS):
            arrived(chip >= distance, piece(distance, 1 - core), chunk)

    group = QUERY_HEAD_COUNT // KEY_VALUE_HEADS
    factor = HEAD_WIDTH ** (-0.5) * math.log2(math.e)

    ones = jnp.ones((keys, HEAD_WIDTH), jnp.bfloat16)
    hidden = bias[...][None]
    for g in range(KEY_VALUE_HEADS):
        first = g * group * HEAD_WIDTH
        queries = jnp.concatenate(
            [q_buf[:, pl.ds(first + h * HEAD_WIDTH, HEAD_WIDTH)] for h in range(group)], axis=0
        )
        key = kv[pl.ds(0, keys), pl.ds(g * HEAD_WIDTH, HEAD_WIDTH)]
        value = kv[pl.ds(0, keys), pl.ds(width + g * HEAD_WIDTH, HEAD_WIDTH)]
        scores = lax.dot_general(
            queries, key, (((1,), (1,)), ((), ())), preferred_element_type=jnp.float32
        )
        scores = (scores.reshape(group, rows, keys) + hidden).reshape(group * rows, keys)
        top = jnp.max(scores, axis=1, keepdims=True)
        probs = jnp.exp2((scores - top) * factor).astype(jnp.bfloat16)
        both = jnp.dot(
            probs, jnp.concatenate([value, ones], axis=1), preferred_element_type=jnp.float32
        )
        out = (both[:, :HEAD_WIDTH] / both[:, HEAD_WIDTH:]).astype(jnp.bfloat16)
        for h in range(group):
            o_ref[:, pl.ds(first + h * HEAD_WIDTH, HEAD_WIDTH)] = out[h * rows : (h + 1) * rows]
    for when, copy in sent:
        pl.when(when)(copy.wait_send)


def body(n_ctx, n_tp, queries, keys, values, doc_starts):
    deep, across, planes, lines = plan(n_ctx, n_tp)
    reach = lines * deep
    rows, width = keys.shape
    pieces = CORES * (reach + 1)
    copies = (lines + 1) * (across + deep + 2 * deep)
    return pl.pallas_call(
        functools.partial(kernel, n_ctx, n_tp, doc_starts.shape[0]),
        out_shape=jax.ShapeDtypeStruct(queries.shape, queries.dtype),
        in_specs=[pl.BlockSpec(memory_space=pltpu.SMEM)]
        + [pl.BlockSpec(memory_space=pltpu.HBM)] * 3,
        out_specs=pl.BlockSpec(memory_space=pltpu.VMEM),
        scratch_shapes=[
            pltpu.VMEM(queries.shape, queries.dtype),
            pltpu.VMEM((pieces * rows, 2 * width), keys.dtype),
            pltpu.VMEM((rows, CORES * rows * (reach + 1)), jnp.float32),
            pltpu.SemaphoreType.DMA((3,)),
            pltpu.SemaphoreType.DMA((copies * CHUNKS,)),
            pltpu.SemaphoreType.DMA((pieces, CHUNKS)),
        ],
        compiler_params=pltpu.CompilerParams(collective_id=0, has_side_effects=True, vmem_limit_bytes=VMEM_BYTES),
    )(doc_starts, queries, keys, values)


def solution(mesh):
    n_ctx, n_tp = mesh.shape["ctx"], mesh.shape["tp"]
    in_specs = (P(("ctx", "tp"), None), P(("ctx", "tp"), None), P(("ctx", "tp"), None), P())
    return jax.shard_map(
        functools.partial(body, n_ctx, n_tp),
        mesh=mesh,
        in_specs=in_specs,
        out_specs=P(("ctx", "tp"), None),
        check_vma=False,
    )
```

```python
import functools
import math

import jax
import jax.numpy as jnp
from jax import lax
from jax.experimental import pallas as pl
from jax.experimental.pallas import tpu as pltpu
from jax.sharding import PartitionSpec as P

QUERY_HEAD_COUNT = 64
KEY_VALUE_HEADS = 8
HEAD_WIDTH = 128
CORES = 2
ROW_CUTS = 2
CHUNKS = 2 * ROW_CUTS
VMEM_BYTES = 67043328 - 540 * 1024
MESH = pl.DeviceIdType.MESH


def plan(n_ctx, n_tp):
    deep = n_tp // CORES
    across = deep if n_ctx % deep == 0 else 1
    return deep, across, n_ctx // across, min(8, n_ctx // 2) - 1


def kernel(n_ctx, n_tp, n_docs, docs, q_hbm, k_hbm, v_hbm, o_ref, q_buf, kv, bias, local_sem, send_sem, recv_sem):
    deep, across, planes, lines = plan(n_ctx, n_tp)
    in_plane, reach = deep * across, lines * deep
    rows = k_hbm.shape[0]
    width = k_hbm.shape[1]
    me = lax.axis_index("ctx") * n_tp + lax.axis_index("tp")
    core, chip = lax.rem(me, CORES), lax.div(me, CORES)
    plane, x = lax.div(chip, in_plane), lax.rem(lax.div(chip, deep), across)
    y = lax.rem(chip, deep)

    def device(other_chip, other_core):
        index = other_chip * CORES + other_core
        return (lax.div(index, n_tp), lax.rem(index, n_tp))

    def piece(distance, from_core):
        return CORES * (reach - distance) + from_core

    tall = rows // ROW_CUTS

    def part(index, chunk):
        cut, side = chunk % ROW_CUTS, chunk // ROW_CUTS
        return kv.at[
            pl.ds(pl.multiple_of(index * rows + cut * tall, tall), tall),
            pl.ds(side * width, width),
        ]

    own = piece(0, core)
    own_rows = pl.ds(pl.multiple_of(own * rows, rows), rows)
    load_k = pltpu.make_async_copy(k_hbm, kv.at[own_rows, pl.ds(0, width)], local_sem.at[0])
    load_v = pltpu.make_async_copy(v_hbm, kv.at[own_rows, pl.ds(width, width)], local_sem.at[1])
    load_q = pltpu.make_async_copy(q_hbm, q_buf, local_sem.at[2])
    load_k.start()
    load_v.start()
    load_q.start()

    partner = device(chip, 1 - core)
    other_x = [lax.rem(x + o, across) for o in range(1, across)]
    other_y = [lax.rem(y + o, deep) for o in range(1, deep)]
    peers = [partner]
    peers += [device(chip + (other - x) * deep, core) for other in other_x]
    peers += [device(chip + other - y, core) for other in other_y]
    barrier = pltpu.get_barrier_semaphore()
    for peer in peers:
        pl.semaphore_signal(barrier, inc=1, device_id=peer, device_id_type=MESH)
    below, above = plane > 0, plane < planes - 1

    @pl.when(below)
    def _():
        pl.semaphore_signal(
            barrier, inc=1, device_id=device(chip - in_plane, core), device_id_type=MESH
        )

    @pl.when(above)
    def _():
        pl.semaphore_signal(
            barrier, inc=1, device_id=device(chip + in_plane, core), device_id_type=MESH
        )

    sent = []

    def send(when, chunk, source, target, target_index):
        copy = pltpu.make_async_remote_copy(
            src_ref=part(source, chunk),
            dst_ref=part(target_index, chunk),
            send_sem=send_sem.at[len(sent)],
            recv_sem=recv_sem.at[target_index, chunk],
            device_id=target,
            device_id_type=MESH,
        )
        sent.append((when, copy))
        pl.when(when)(copy.start)

    def arrived(when, index, chunk):
        place = part(index, chunk)
        copy = pltpu.make_async_copy(place, place, recv_sem.at[index, chunk])
        pl.when(when)(copy.wait)

    for distance in range(1, reach + 1):
        @pl.when(chip < distance)
        def _():
            first = piece(distance, 0) * rows
            kv[pl.ds(first, CORES * rows), :] = jnp.zeros((CORES * rows, 2 * width), kv.dtype)

    pl.semaphore_wait(
        barrier, len(peers) + below.astype(jnp.int32) + above.astype(jnp.int32)
    )

    def hand_on(line, chunk):
        index = piece(line * deep, core)
        held = chip >= line * deep
        if line + across <= lines:
            straight = held if line == 0 else held & (line > x)
            send(straight & above, chunk, index, device(chip + in_plane, core),
                 piece((line + across) * deep, core))
        if line in (0, across):
            for other in other_x:
                away = line + other - x
                send(held & (away >= 1) & (away <= lines), chunk, index,
                     device(chip + (other - x) * deep, core),
                     piece(jnp.clip(away, 1, lines) * deep, core))
        for other in other_y:
            away = line * deep + other - y
            wanted = held & (away >= 1) & (away <= reach)
            if across > 1:
                if line == 1:
                    wanted &= x > 0
                wanted &= (x < across - 1) | (away < in_plane) | (away >= in_plane + deep)
            send(wanted, chunk, index,
                 device(chip + other - y, core), piece(jnp.clip(away, 1, reach), core))
        send(held, chunk, index, partner, index)

    def line_in(line):
        for chunk in range(CHUNKS):
            arrived(chip >= line * deep, piece(line * deep, core), chunk)
            hand_on(line, chunk)

    def beside(line):
        for off in range(1 - deep, deep):
            back = line * deep + off
            if off and 1 <= back <= reach:
                when = (chip >= back) & (y - off >= 0) & (y - off < deep)
                index = piece(back, core)
                for chunk in range(CHUNKS):
                    arrived(when, index, chunk)
                    last = when & (x == across - 1)
                    if across > 1 and back < deep and back + in_plane <= reach:
                        send(last & above, chunk, index, device(chip + in_plane, core),
                             piece(back + in_plane, core))
                    if across > 1 and line == across:
                        send(last, chunk, index, device(chip - (across - 1) * deep, core),
                             piece(deep + off, core))
                    send(when, chunk, index, partner, index)

    load_k.wait()
    for chunk in range(CHUNKS):
        if chunk == ROW_CUTS:
            load_v.wait()
        hand_on(0, chunk)

    keys = CORES * rows * (reach + 1)
    query_pos = me * rows + lax.broadcasted_iota(jnp.int32, (rows, keys), 0)
    key_pos = (chip - reach) * (CORES * rows) + lax.broadcasted_iota(jnp.int32, (rows, keys), 1)
    token = me * rows + lax.broadcasted_iota(jnp.int32, (rows, 1), 0)
    begin = jnp.zeros((rows, 1), jnp.int32)
    for doc in range(n_docs):
        start = docs[doc]
        begin = jnp.maximum(begin, jnp.where(start <= token, start, 0))
    visible = (key_pos <= query_pos) & (key_pos >= begin)
    bias[...] = jnp.where(visible, 0.0, -1e30)
    load_q.wait()

    line_in(across)
    beside(0)
    for line in range(1, across):
        line_in(line)
    beside(across)
    for line in range(1, across):
        beside(line)
    for line in range(across + 1, lines + 1):
        line_in(line)
    for line in range(across + 1, lines + 1):
        beside(line)
    for distance in range(reach + 1):
        for chunk in range(CHUNKS):
            arrived(chip >= distance, piece(distance, 1 - core), chunk)

    group = QUERY_HEAD_COUNT // KEY_VALUE_HEADS
    factor = HEAD_WIDTH ** (-0.5) * math.log2(math.e)

    ones = jnp.ones((keys, HEAD_WIDTH), jnp.bfloat16)
    hidden = bias[...][None]
    for g in range(KEY_VALUE_HEADS):
        first = g * group * HEAD_WIDTH
        queries = jnp.concatenate(
            [q_buf[:, pl.ds(first + h * HEAD_WIDTH, HEAD_WIDTH)] for h in range(group)], axis=0
        )
        key = kv[pl.ds(0, keys), pl.ds(g * HEAD_WIDTH, HEAD_WIDTH)]
        value = kv[pl.ds(0, keys), pl.ds(width + g * HEAD_WIDTH, HEAD_WIDTH)]
        scores = lax.dot_general(
            queries, key, (((1,), (1,)), ((), ())), preferred_element_type=jnp.float32
        )
        scores = (scores.reshape(group, rows, keys) + hidden).reshape(group * rows, keys)
        top = jnp.max(scores, axis=1, keepdims=True)
        probs = jnp.exp2((scores - top) * factor).astype(jnp.bfloat16)
        both = jnp.dot(
            probs, jnp.concatenate([value, ones], axis=1), preferred_element_type=jnp.float32
        )
        out = (both[:, :HEAD_WIDTH] / both[:, HEAD_WIDTH:]).astype(jnp.bfloat16)
        for h in range(group):
            o_ref[:, pl.ds(first + h * HEAD_WIDTH, HEAD_WIDTH)] = out[h * rows : (h + 1) * rows]
    for when, copy in sent:
        pl.when(when)(copy.wait_send)


def body(n_ctx, n_tp, queries, keys, values, doc_starts):
    deep, across, planes, lines = plan(n_ctx, n_tp)
    reach = lines * deep
    rows, width = keys.shape
    pieces = CORES * (reach + 1)
    copies = (lines + 1) * 3 * deep + 2 * across + 4 * deep
    return pl.pallas_call(
        functools.partial(kernel, n_ctx, n_tp, doc_starts.shape[0]),
        out_shape=jax.ShapeDtypeStruct(queries.shape, queries.dtype),
        in_specs=[pl.BlockSpec(memory_space=pltpu.SMEM)]
        + [pl.BlockSpec(memory_space=pltpu.HBM)] * 3,
        out_specs=pl.BlockSpec(memory_space=pltpu.VMEM),
        scratch_shapes=[
            pltpu.VMEM(queries.shape, queries.dtype),
            pltpu.VMEM((pieces * rows, 2 * width), keys.dtype),
            pltpu.VMEM((rows, CORES * rows * (reach + 1)), jnp.float32),
            pltpu.SemaphoreType.DMA((3,)),
            pltpu.SemaphoreType.DMA((copies * CHUNKS,)),
            pltpu.SemaphoreType.DMA((pieces, CHUNKS)),
        ],
        compiler_params=pltpu.CompilerParams(collective_id=0, has_side_effects=True, vmem_limit_bytes=VMEM_BYTES),
    )(doc_starts, queries, keys, values)


def solution(mesh):
    n_ctx, n_tp = mesh.shape["ctx"], mesh.shape["tp"]
    in_specs = (P(("ctx", "tp"), None), P(("ctx", "tp"), None), P(("ctx", "tp"), None), P())
    return jax.shard_map(
        functools.partial(body, n_ctx, n_tp),
        mesh=mesh,
        in_specs=in_specs,
        out_specs=P(("ctx", "tp"), None),
        check_vma=False,
    )
```
